1024 devices in a mesh: replica: 64 (over z_hi, y, core), shard: 16 (over x, z_lo).
Axes of the slice: x: 4, y: 8, z: 16 (z_hi: 4, z_lo: 4; z = z_hi * 4 + z_lo), core: 2. Of those that a mesh axis runs over, the one named last changes fastest.
Arguments:
- deltas: bfloat16 [64, 4194304], P('replica', 'shard'), may hold values from -16 to 16
- counts: int32 [32], replicated, may hold values from 1000 to 8999, as said below
- momentum: float32 [8388608], P(('shard', 'replica')), may hold values from -4 to 4
- params: bfloat16 [8388608], P(('shard', 'replica')), may hold values from -6 to 6
Outputs:
- new_momentum: float32 [8388608], P(('shard', 'replica'))
- new_params: bfloat16 [8388608], P('shard')
The draws below stay inside these ranges and needn't reach their ends.
Inputs may be any that keep to these rules, and one draw needn't show every extreme that they name: `counts`: tokens processed by each worker.
All inputs are finite; a program needn't handle non-finite values.
Results may differ from the reference program's by a relative error of at most 0.001.
Values may be sent and summed in bfloat16 or wider, within the bound.
No kernel may reach another device: no remote copies, remote signals or barrier semaphores. Data moves between devices by JAX's collectives and lax.ppermute only.
A program may use at most 32 MiB of HBM per device.

```python
import jax
import jax.numpy as jnp
from jax import lax

REPLICAS = 32
TOTAL = 8388608
HALF = 4194304
N_REPLICA = 64
N_SHARD = 16


def draw_counts(key, part):
    base = jax.random.randint(jax.random.fold_in(key, 11), (REPLICAS,), 1000, 3000)
    steps = jnp.arange(REPLICAS, dtype=jnp.int32)
    rising = (base * (REPLICAS - 1 + 2 * steps) // (REPLICAS - 1)).astype(jnp.int32)
    rising = jnp.where(steps == 0, 1000, rising)
    rising = jnp.where(steps == REPLICAS - 1, 8999, rising)
    return rising.astype(jnp.int32)


def spiked(values, stream_key, source, target, shards_of, factor):
    def block_of(axis_at):
        return (jnp.arange(values.shape[axis_at]) // (values.shape[axis_at] // shards_of)).reshape((-1,) + (1,) * (values.ndim - 1 - axis_at))

    near = jax.random.permutation(stream_key, shards_of)[block_of(target)]
    far = (block_of(target) + shards_of // 2) % shards_of
    return jnp.where((block_of(source) == near) | (block_of(source) == far), factor * values, values)


def level_of(rng, extent, split, smallest, high):
    def one(axis_at, blocks):
        draws = jax.random.uniform(jax.random.fold_in(jax.random.fold_in(rng, 6), axis_at), (blocks,), jnp.float32, smallest / len(split), high / len(split))
        return jnp.repeat(jnp.exp(draws), extent[axis_at] // blocks).reshape((-1,) + (1,) * (len(extent) - axis_at - 1))

    gain = one(*split[0])
    for cut in split[1:]:
        gain = gain * one(*cut)
    return gain


def gaussian(key, shape, deviation, reach, shards=(), held_as=jnp.bfloat16):
    result = jax.random.normal(key, shape, jnp.float32) * deviation
    if len(shards) > 0:
        result = level_of(key, shape, shards, -0.22, 0.18) * result
    return jnp.clip(result, min=-reach, max=reach).astype(held_as)


def gaussian_with(rng, shape, width, reach, cuts, heavy, kind=jnp.bfloat16):
    drawn = width * jax.random.normal(rng, shape, jnp.float32)
    if cuts:
        drawn = drawn * level_of(rng, shape, cuts, -0.22, 0.18)
    return jnp.clip(spiked(drawn, jax.random.fold_in(rng, 3), *heavy), -reach, reach).astype(kind)


def setup_inputs(seed: int = 0) -> dict:
    arg_keys = jax.random.split(jax.random.key(seed), 5)
    return {
        "deltas": gaussian_with(arg_keys[0], (N_REPLICA, HALF), 1.0, 16.0, ((0, 64), (1, 16)), (0, 1, 64, 4.0)),
        "counts": draw_counts(jax.random.fold_in(arg_keys[4], 71), 0),
        "momentum": gaussian(arg_keys[2], (TOTAL,), 0.3, 4.0, ((0, 1024),), jnp.float32),
        "params": gaussian(arg_keys[3], (TOTAL,), 1.0, 6.0, ((0, 1024),)),
    }


momentum_rate = 0.9
outer_rate = 0.7


def reference(deltas, counts, momentum, params):
    workers = deltas.shape[0] // 2
    stacked = deltas.reshape(workers, 2, N_SHARD, deltas.shape[1] // N_SHARD)
    worker_delta = jnp.transpose(stacked, (0, 2, 1, 3)).reshape(workers, momentum.shape[0])
    shares = counts.astype(jnp.float32)
    shares = shares / jnp.sum(shares)

    def accumulate(total, item):
        row, share = item
        return total + share * row.astype(jnp.float32), None

    outer_grad, _ = lax.scan(accumulate, jnp.zeros((momentum.shape[0],), jnp.float32), (worker_delta, shares))
    new_momentum = momentum_rate * momentum + outer_grad
    new_params = (params.astype(jnp.float32) - outer_rate * (outer_grad + momentum_rate * new_momentum)).astype(jnp.bfloat16)
    return new_momentum, new_params
```

```python
import jax
import jax.numpy as jnp
from jax import lax
from jax.sharding import Mesh
from jax.sharding import PartitionSpec as P

momentum_rate = 0.9
outer_rate = 0.7


def local(deltas, counts, momentum, params):
    nz, ny, nc = lax.axis_size("z"), lax.axis_size("y"), lax.axis_size("c")
    workers = nz * ny
    z, y = lax.axis_index("z"), lax.axis_index("y")
    piece = momentum.shape[0]
    rows = piece // 128
    shares = counts.astype(jnp.float32)
    shares = shares / jnp.sum(shares)

    wide = lax.optimization_barrier(deltas.astype(jnp.float32))
    narrow = wide.reshape(deltas.shape[1] // 128, 128).astype(jnp.bfloat16)
    blocks = narrow.reshape(nz // 2, ny, nc, rows, 128)

    def sent(j):
        out = lax.dynamic_index_in_dim(blocks, (y + j) % ny, 1, keepdims=False)
        if j:
            out = lax.ppermute(out, "y", [(i, (i + j) % ny) for i in range(ny)])
        share = lax.dynamic_index_in_dim(shares, z * ny + (y - j) % ny, 0, keepdims=False)
        return share, out

    terms = [sent(j) for j in range(ny)]
    partial = sum(share * got.astype(jnp.float32) for share, got in terms)
    partial = partial.reshape(nz, rows, 128)

    def joined(j):
        perm = []
        for zi in range(nz):
            for h in range(nc):
                q = zi ^ j
                perm.append((zi * nc + h, ((nz // 2) * h + q // nc) * nc + q % nc))
        mine = lax.dynamic_index_in_dim(partial, z ^ j, 0, keepdims=False)
        return lax.ppermute(mine, ("z", "c"), perm)

    outer_grad = sum(joined(j) for j in range(nz))
    new_momentum = momentum_rate * momentum.reshape(rows, 128) + outer_grad
    updated = (
        params.reshape(rows, 128).astype(jnp.float32)
        - outer_rate * (outer_grad + momentum_rate * new_momentum)
    ).astype(jnp.bfloat16)

    def gathered(x, axis):
        n = lax.axis_size(axis)
        at = lax.axis_index(axis)
        parts = [x] + [
            lax.ppermute(x, axis, [(i, (i + j) % n) for i in range(n)]) for j in range(1, n)
        ]
        out = jnp.zeros((n, *x.shape), x.dtype)
        for j, p in enumerate(parts):
            out = lax.dynamic_update_index_in_dim(out, p, (at - j) % n, 0)
        return out

    zs = gathered(updated, "z")
    ys = gathered(zs, "y")
    cs = gathered(ys, "c")
    whole = jnp.transpose(cs, (2, 1, 0, 3, 4))
    return new_momentum.reshape(piece), whole.reshape(-1)


def solution(mesh):
    torus = Mesh(mesh.devices.reshape(4, 8, 2, mesh.shape["shard"]), ("z", "y", "c", "shard"))
    R = ("z", "y", "c")
    return jax.shard_map(
        local,
        mesh=torus,
        in_specs=(P(R, "shard"), P(), P(("shard",) + R), P(("shard",) + R)),
        out_specs=(P(("shard",) + R), P("shard")),
        check_vma=False,
    )
```

```python
import jax
import jax.numpy as jnp
from jax import lax
from jax.experimental import pallas as pl
from jax.experimental.pallas import tpu as pltpu
from jax.sharding import Mesh
from jax.sharding import PartitionSpec as P

momentum_rate = 0.9
outer_rate = 0.7
READS = 4

VMEM = pl.BlockSpec(memory_space=pltpu.VMEM)
SMEM = pl.BlockSpec(memory_space=pltpu.SMEM)
HBM = pl.BlockSpec(memory_space=pltpu.HBM)


def on_chip(x):
    return pltpu.with_memory_space_constraint(x, pltpu.VMEM)


def prepared(deltas, counts, momentum, params, z, ny, nc, nz):
    rows = momentum.shape[0]
    pairs, planes = ny * nc, nz // nc
    step = deltas.shape[1] // READS
    pieces_of = step // (rows * 128)
    workers = counts.shape[0]

    def body(z_ref, counts_ref, src, old, was, out, shares_ref, old_ref, was_ref, held, sems):
        reads = [
            pltpu.make_async_copy(
                src.at[:, pl.ds(k * step, step)], held.at[:, pl.ds(k * step, step)], sems.at[k]
            )
            for k in range(READS)
        ]
        for read in reads:
            read.start()
        rest = [
            pltpu.make_async_copy(old, old_ref, sems.at[READS]),
            pltpu.make_async_copy(was, was_ref, sems.at[READS + 1]),
        ]
        for read in rest:
            read.start()
        total = counts_ref[0]
        for w in range(1, workers):
            total += counts_ref[w]
        whole = jnp.full((8, 128), total, jnp.int32).astype(jnp.float32)
        first = z_ref[0] * ny
        for y in range(ny):
            count = jnp.full((8, 128), counts_ref[first + y], jnp.int32).astype(jnp.float32)
            shares_ref[y] = count / whole
        for k, read in enumerate(reads):
            read.wait()
            for piece in range(k * pieces_of, (k + 1) * pieces_of):
                at = piece * rows * 128
                block = held[:, at : at + rows * 128].astype(jnp.float32).reshape(rows, 128)
                out[piece % pairs, piece // pairs] = block.astype(jnp.bfloat16)
        for read in rest:
            read.wait()

    return pl.pallas_call(
        body,
        out_shape=[
            pltpu.VMEM((pairs, planes, rows, 128), jnp.bfloat16),
            pltpu.VMEM((ny, 8, 128), jnp.float32),
            pltpu.VMEM((rows, 128), momentum.dtype),
            pltpu.VMEM((rows, 128), params.dtype),
        ],
        in_specs=[SMEM, SMEM, HBM, HBM, HBM],
        out_specs=[VMEM] * 4,
        scratch_shapes=[
            pltpu.VMEM(deltas.shape, deltas.dtype),
            pltpu.SemaphoreType.DMA((READS + 2,)),
        ],
        name="prepared",
    )(z.reshape(1), counts, deltas, momentum, params)


def weighted(got, shares, nc):
    pairs, planes, rows, _ = got.shape

    def body(shares_ref, got_ref, out_ref):
        shares = [shares_ref[y][None] for y in range(pairs // nc)]
        for h in range(nc):
            for p in range(planes):
                acc = None
                for y, share in enumerate(shares):
                    term = got_ref[y * nc + h, p].astype(jnp.float32).reshape(rows // 8, 8, 128)
                    term = share * term
                    acc = term if acc is None else acc + term
                out_ref[h * planes + p] = acc.reshape(rows, 128)

    return pl.pallas_call(
        body,
        out_shape=pltpu.VMEM((nc * planes, rows, 128), jnp.float32),
        in_specs=[VMEM, VMEM],
        out_specs=VMEM,
        name="weighted",
    )(on_chip(shares), on_chip(got))


def updated(got, old, was):
    planes, rows, _ = got.shape

    def body(got_ref, old_ref, was_ref, momentum_ref, out_ref):
        grad = got_ref[0]
        for z in range(1, planes):
            grad = grad + got_ref[z]
        m = momentum_rate * old_ref[...] + grad
        momentum_ref[...] = m
        new = was_ref[...].astype(jnp.float32) - outer_rate * (grad + momentum_rate * m)
        new = new.astype(jnp.bfloat16)
        for z in range(planes):
            out_ref[z] = new

    return pl.pallas_call(
        body,
        out_shape=[
            pltpu.VMEM((rows, 128), jnp.float32),
            pltpu.VMEM((planes, rows, 128), jnp.bfloat16),
        ],
        in_specs=[VMEM] * 3,
        out_specs=[VMEM] * 2,
        name="updated",
    )(on_chip(got), on_chip(old), on_chip(was))


def exchanged(x, axes):
    return lax.all_to_all(x, axes, 0, 0, tiled=True)


def local(deltas, counts, momentum, params):
    nz, ny, nc = lax.axis_size("z"), lax.axis_size("y"), lax.axis_size("c")
    z, c = lax.axis_index("z"), lax.axis_index("c")
    rows = momentum.shape[0] // 128

    pieces, shares, old, was = prepared(
        deltas, counts, momentum.reshape(rows, 128), params.reshape(rows, 128), z, ny, nc, nz
    )
    partial = weighted(exchanged(pieces, ("y", "c")), shares, nc)
    new_momentum, copies = updated(exchanged(partial, "z"), old, was)
    plane = exchanged(copies, "z")
    own = exchanged(jnp.broadcast_to(plane[None], (ny, *plane.shape)), "y")
    other = lax.ppermute(own, "c", [(0, 1), (1, 0)])

    out = jnp.zeros((nz, ny, nc, rows, 128), jnp.bfloat16)
    for at, half in ((c, own), (1 - c, other)):
        block = jnp.swapaxes(half, 0, 1)[:, :, None]
        out = lax.dynamic_update_slice(out, block, (0, 0, at, 0, 0))
    return new_momentum.reshape(-1), out.reshape(-1)


def solution(mesh):
    torus = Mesh(mesh.devices.reshape(4, 8, 2, mesh.shape["shard"]), ("z", "y", "c", "shard"))
    R = ("z", "y", "c")
    return jax.shard_map(
        local,
        mesh=torus,
        in_specs=(P(R, "shard"), P(), P(("shard",) + R), P(("shard",) + R)),
        out_specs=(P(("shard",) + R), P("shard")),
        check_vma=False,
    )
```

```python
import jax
import jax.numpy as jnp
from jax import lax
from jax.experimental import pallas as pl
from jax.experimental.pallas import tpu as pltpu
from jax.sharding import Mesh
from jax.sharding import PartitionSpec as P

momentum_rate = 0.9
outer_rate = 0.7
grad_rate = outer_rate * (1 + momentum_rate)
old_rate = outer_rate * momentum_rate * momentum_rate
READS = 4

VMEM = pl.BlockSpec(memory_space=pltpu.VMEM)
SMEM = pl.BlockSpec(memory_space=pltpu.SMEM)
HBM = pl.BlockSpec(memory_space=pltpu.HBM)


def on_chip(x):
    return pltpu.with_memory_space_constraint(x, pltpu.VMEM)


def prepared(deltas, counts, momentum, params, z, ny, nc, nz):
    rows = momentum.shape[0]
    pairs, planes = ny * nc, nz // nc
    step = deltas.shape[1] // READS
    pieces_of = step // (rows * 128)
    workers = counts.shape[0]

    def body(z_ref, counts_ref, src, old, was, out, shares_ref, old_ref, was_ref, held, sems):
        reads = [
            pltpu.make_async_copy(
                src.at[:, pl.ds(k * step, step)], held.at[:, pl.ds(k * step, step)], sems.at[k]
            )
            for k in range(READS)
        ]
        for read in reads:
            read.start()
        rest = [
            pltpu.make_async_copy(old, old_ref, sems.at[READS]),
            pltpu.make_async_copy(was, was_ref, sems.at[READS + 1]),
        ]
        for read in rest:
            read.start()
        total = counts_ref[0]
        for w in range(1, workers):
            total += counts_ref[w]
        whole = jnp.full((8, 128), total, jnp.int32).astype(jnp.float32)
        first = z_ref[0] * ny
        for y in range(ny):
            count = jnp.full((8, 128), counts_ref[first + y], jnp.int32).astype(jnp.float32)
            shares_ref[y] = count / whole
        for k, read in enumerate(reads):
            read.wait()
            for piece in range(k * pieces_of, (k + 1) * pieces_of):
                at = piece * rows * 128
                block = held[:, at : at + rows * 128].astype(jnp.float32).reshape(rows, 128)
                out[piece % pairs, piece // pairs] = block.astype(jnp.bfloat16)
        for read in rest:
            read.wait()

    return pl.pallas_call(
        body,
        out_shape=[
            pltpu.VMEM((pairs, planes, rows, 128), jnp.bfloat16),
            pltpu.VMEM((ny, 8, 128), jnp.float32),
            pltpu.VMEM((rows, 128), momentum.dtype),
            pltpu.VMEM((rows, 128), params.dtype),
        ],
        in_specs=[SMEM, SMEM, HBM, HBM, HBM],
        out_specs=[VMEM] * 4,
        scratch_shapes=[
            pltpu.VMEM(deltas.shape, deltas.dtype),
            pltpu.SemaphoreType.DMA((READS + 2,)),
        ],
        name="prepared",
    )(z.reshape(1), counts, deltas, momentum, params)


def weighted(got, shares, old, was, z, nc):
    pairs, planes, rows, _ = got.shape

    def body(z_ref, shares_ref, got_ref, old_ref, was_ref, out_ref, own_ref):
        shares = [shares_ref[y][None] for y in range(pairs // nc)]
        for h in range(nc):
            for p in range(planes):
                acc = None
                for y, share in enumerate(shares):
                    term = got_ref[y * nc + h, p].astype(jnp.float32).reshape(rows // 8, 8, 128)
                    term = share * term
                    acc = term if acc is None else acc + term
                out_ref[h * planes + p] = acc.reshape(rows, 128)
        z = z_ref[0]
        own = out_ref[z]
        own_ref[...] = own
        rest = was_ref[...].astype(jnp.float32) * (1 / grad_rate) - old_ref[...] * (old_rate / grad_rate)
        out_ref[z] = own - rest

    return pl.pallas_call(
        body,
        out_shape=[
            pltpu.VMEM((nc * planes, rows, 128), jnp.float32),
            pltpu.VMEM((rows, 128), jnp.float32),
        ],
        in_specs=[SMEM] + [VMEM] * 4,
        out_specs=[VMEM] * 2,
        name="weighted",
    )(z.reshape(1), *map(on_chip, (shares, got, old, was)))


def updated(every, own, old, z):
    planes, _, rows, _ = every.shape

    def body(z_ref, every_ref, own_ref, old_ref, momentum_ref, out_ref):
        z = z_ref[0]
        grad = own_ref[...]
        for step in range(1, planes):
            grad = grad + every_ref[(z + step) % planes, z]
        momentum_ref[...] = momentum_rate * old_ref[...] + grad
        for p in range(planes):
            total = every_ref[0, p]
            for k in range(1, planes):
                total = total + every_ref[k, p]
            out_ref[p] = (-grad_rate * total).astype(jnp.bfloat16)

    return pl.pallas_call(
        body,
        out_shape=[
            pltpu.VMEM((rows, 128), jnp.float32),
            pltpu.VMEM((planes, rows, 128), jnp.bfloat16),
        ],
        in_specs=[SMEM] + [VMEM] * 3,
        out_specs=[VMEM] * 2,
        name="updated",
    )(z.reshape(1), *map(on_chip, (every, own, old)))


def exchanged(x, axes):
    return lax.all_to_all(x, axes, 0, 0, tiled=True)


def local(deltas, counts, momentum, params):
    nz, ny, nc = lax.axis_size("z"), lax.axis_size("y"), lax.axis_size("c")
    z, c = lax.axis_index("z"), lax.axis_index("c")
    rows = momentum.shape[0] // 128

    pieces, shares, old, was = prepared(
        deltas, counts, momentum.reshape(rows, 128), params.reshape(rows, 128), z, ny, nc, nz
    )
    partial, mine = weighted(exchanged(pieces, ("y", "c")), shares, old, was, z, nc)
    new_momentum, plane = updated(lax.all_gather(partial, "z"), mine, old, z)
    own = exchanged(jnp.broadcast_to(plane[None], (ny, *plane.shape)), "y")
    other = lax.ppermute(own, "c", [(0, 1), (1, 0)])

    out = jnp.zeros((nz, ny, nc, rows, 128), jnp.bfloat16)
    for at, half in ((c, own), (1 - c, other)):
        block = jnp.swapaxes(half, 0, 1)[:, :, None]
        out = lax.dynamic_update_slice(out, block, (0, 0, at, 0, 0))
    return new_momentum.reshape(-1), out.reshape(-1)


def solution(mesh):
    torus = Mesh(mesh.devices.reshape(4, 8, 2, mesh.shape["shard"]), ("z", "y", "c", "shard"))
    R = ("z", "y", "c")
    return jax.shard_map(
        local,
        mesh=torus,
        in_specs=(P(R, "shard"), P(), P(("shard",) + R), P(("shard",) + R)),
        out_specs=(P(("shard",) + R), P("shard")),
        check_vma=False,
    )
```

```python
import jax
import jax.numpy as jnp
from jax import lax
from jax.experimental import pallas as pl
from jax.experimental.pallas import tpu as pltpu
from jax.sharding import Mesh
from jax.sharding import PartitionSpec as P

momentum_rate = 0.9
outer_rate = 0.7
grad_rate = outer_rate * (1 + momentum_rate)
old_rate = outer_rate * momentum_rate * momentum_rate
READS = 4
Y_ORDER = (0, 4, 2, 6, 1, 5, 3, 7)
CORES = 2
ALL_ORDER = [y * CORES + c for c in range(CORES) for y in Y_ORDER]
SAME_CORE = [[y * CORES + c for y in Y_ORDER] for c in range(CORES)]

VMEM = pl.BlockSpec(memory_space=pltpu.VMEM)
SMEM = pl.BlockSpec(memory_space=pltpu.SMEM)
HBM = pl.BlockSpec(memory_space=pltpu.HBM)


def on_chip(x):
    return pltpu.with_memory_space_constraint(x, pltpu.VMEM)


def prepared(deltas, counts, momentum, params, z, ny, nc, nz):
    rows = momentum.shape[0]
    pairs, planes = ny * nc, nz // nc
    step = deltas.shape[1] // READS
    pieces_of = step // (rows * 128)
    workers = counts.shape[0]

    def body(z_ref, counts, src, old, was, out, shares_ref, old_ref, was_ref, held, counts_ref, sems):
        reads = [
            pltpu.make_async_copy(
                src.at[:, pl.ds(k * step, step)], held.at[:, pl.ds(k * step, step)], sems.at[k]
            )
            for k in range(READS)
        ]
        for read in reads:
            read.start()
        tokens = pltpu.make_async_copy(counts, counts_ref, sems.at[READS + 2])
        tokens.start()
        rest = [
            pltpu.make_async_copy(old, old_ref, sems.at[READS]),
            pltpu.make_async_copy(was, was_ref, sems.at[READS + 1]),
        ]
        for read in rest:
            read.start()
        tokens.wait()
        total = counts_ref[0]
        for w in range(1, workers):
            total += counts_ref[w]
        whole = jnp.full((8, 128), total, jnp.int32).astype(jnp.float32)
        first = z_ref[0] * ny
        for y in range(ny):
            count = jnp.full((8, 128), counts_ref[first + y], jnp.int32).astype(jnp.float32)
            shares_ref[y] = count / whole
        for k, read in enumerate(reads):
            read.wait()
            for piece in range(k * pieces_of, (k + 1) * pieces_of):
                at = piece * rows * 128
                block = held[:, at : at + rows * 128].astype(jnp.float32).reshape(rows, 128)
                out[ALL_ORDER.index(piece % pairs), piece // pairs] = block.astype(jnp.bfloat16)
        for read in rest:
            read.wait()

    return pl.pallas_call(
        body,
        out_shape=[
            pltpu.VMEM((pairs, planes, rows, 128), jnp.bfloat16),
            pltpu.VMEM((ny, 8, 128), jnp.float32),
            pltpu.VMEM((rows, 128), momentum.dtype),
            pltpu.VMEM((rows, 128), params.dtype),
        ],
        in_specs=[SMEM, HBM, HBM, HBM, HBM],
        out_specs=[VMEM] * 4,
        scratch_shapes=[
            pltpu.VMEM(deltas.shape, deltas.dtype),
            pltpu.SMEM(counts.shape, counts.dtype),
            pltpu.SemaphoreType.DMA((READS + 3,)),
        ],
        name="prepared",
    )(z.reshape(1), counts, deltas, momentum, params)


def weighted(got, shares, old, was, z, nc):
    pairs, planes, rows, _ = got.shape

    def body(z_ref, shares_ref, got_ref, old_ref, was_ref, out_ref, own_ref):
        shares = [shares_ref[y][None] for y in range(pairs // nc)]
        for h in range(nc):
            for p in range(planes):
                acc = None
                for y, share in enumerate(shares):
                    term = got_ref[ALL_ORDER.index(y * nc + h), p].astype(jnp.float32).reshape(rows // 8, 8, 128)
                    term = share * term
                    acc = term if acc is None else acc + term
                out_ref[h * planes + p] = acc.reshape(rows, 128)
        z = z_ref[0]
        own = out_ref[z]
        own_ref[...] = own
        rest = was_ref[...].astype(jnp.float32) * (1 / grad_rate) - old_ref[...] * (old_rate / grad_rate)
        out_ref[z] = own - rest

    return pl.pallas_call(
        body,
        out_shape=[
            pltpu.VMEM((nc * planes, rows, 128), jnp.float32),
            pltpu.VMEM((rows, 128), jnp.float32),
        ],
        in_specs=[SMEM] + [VMEM] * 4,
        out_specs=[VMEM] * 2,
        name="weighted",
    )(z.reshape(1), *map(on_chip, (shares, got, old, was)))


def updated(every, own, old, z):
    planes, _, rows, _ = every.shape

    def body(z_ref, every_ref, own_ref, old_ref, momentum_ref, out_ref):
        z = z_ref[0]
        grad = own_ref[...]
        for step in range(1, planes):
            grad = grad + every_ref[(z + step) % planes, z]
        momentum_ref[...] = momentum_rate * old_ref[...] + grad
        for p in range(planes):
            total = every_ref[0, p]
            for k in range(1, planes):
                total = total + every_ref[k, p]
            out_ref[p] = (-grad_rate * total).astype(jnp.bfloat16)

    return pl.pallas_call(
        body,
        out_shape=[
            pltpu.VMEM((rows, 128), jnp.float32),
            pltpu.VMEM((planes, rows, 128), jnp.bfloat16),
        ],
        in_specs=[SMEM] + [VMEM] * 3,
        out_specs=[VMEM] * 2,
        name="updated",
    )(z.reshape(1), *map(on_chip, (every, own, old)))


def exchanged(x, groups):
    return lax.all_to_all(x, "yc", 0, 0, tiled=True, axis_index_groups=groups)


def local(deltas, counts, momentum, params):
    nz, nc = lax.axis_size("z"), CORES
    ny = lax.axis_size("yc") // nc
    z, c = lax.axis_index("z"), lax.axis_index("yc") % nc
    rows = momentum.shape[0] // 128

    pieces, shares, old, was = prepared(
        deltas, counts, momentum.reshape(rows, 128), params.reshape(rows, 128), z, ny, nc, nz
    )
    partial, mine = weighted(exchanged(pieces, [ALL_ORDER]), shares, old, was, z, nc)
    new_momentum, plane = updated(lax.all_gather(partial, "z"), mine, old, z)
    own = exchanged(jnp.broadcast_to(plane[None], (ny, *plane.shape)), SAME_CORE)
    other = lax.ppermute(own, "yc", [(i, i ^ 1) for i in range(ny * nc)])

    out = jnp.zeros((nz, ny, nc, rows, 128), jnp.bfloat16)
    for at, half in ((c, own), (1 - c, other)):
        bits = half.reshape(2, 2, 2, nz, rows, 128)
        block = jnp.transpose(bits, (3, 2, 1, 0, 4, 5)).reshape(nz, ny, 1, rows, 128)
        out = lax.dynamic_update_slice(out, block, (0, 0, at, 0, 0))
    return new_momentum.reshape(-1), out.reshape(-1)


def solution(mesh):
    torus = Mesh(mesh.devices.reshape(4, 16, mesh.shape["shard"]), ("z", "yc", "shard"))
    R = ("z", "yc")
    return jax.shard_map(
        local,
        mesh=torus,
        in_specs=(P(R, "shard"), P(), P(("shard",) + R), P(("shard",) + R)),
        out_specs=(P(("shard",) + R), P("shard")),
        check_vma=False,
    )
```

```python
import jax
import jax.numpy as jnp
from jax import lax
from jax.experimental import pallas as pl
from jax.experimental.pallas import tpu as pltpu
from jax.sharding import Mesh
from jax.sharding import PartitionSpec as P

momentum_rate = 0.9
outer_rate = 0.7
grad_rate = outer_rate * (1 + momentum_rate)
old_rate = outer_rate * momentum_rate * momentum_rate
READS = 4
Y_ORDER = (0, 4, 2, 6, 1, 5, 3, 7)
CORES = 2
ALL_ORDER = [y * CORES + c for c in range(CORES) for y in Y_ORDER[:: 1 - 2 * c]]
SAME_CORE = [[y * CORES + c for y in Y_ORDER] for c in range(CORES)]

VMEM = pl.BlockSpec(memory_space=pltpu.VMEM)
SMEM = pl.BlockSpec(memory_space=pltpu.SMEM)
HBM = pl.BlockSpec(memory_space=pltpu.HBM)


def on_chip(x):
    return pltpu.with_memory_space_constraint(x, pltpu.VMEM)


def prepared(deltas, counts, momentum, params, z, ny, nc, nz):
    rows = momentum.shape[0]
    pairs, planes = ny * nc, nz // nc
    step = deltas.shape[1] // READS
    pieces_of = step // (rows * 128)
    workers = counts.shape[0]

    def body(z_ref, counts, src, old, was, out, shares_ref, old_ref, was_ref, held, counts_ref, sems):
        reads = [
            pltpu.make_async_copy(
                src.at[:, pl.ds(k * step, step)], held.at[:, pl.ds(k * step, step)], sems.at[k]
            )
            for k in range(READS)
        ]
        for read in reads:
            read.start()
        tokens = pltpu.make_async_copy(counts, counts_ref, sems.at[READS + 2])
        tokens.start()
        rest = [
            pltpu.make_async_copy(old, old_ref, sems.at[READS]),
            pltpu.make_async_copy(was, was_ref, sems.at[READS + 1]),
        ]
        for read in rest:
            read.start()
        tokens.wait()
        total = counts_ref[0]
        for w in range(1, workers):
            total += counts_ref[w]
        whole = jnp.full((8, 128), total, jnp.int32).astype(jnp.float32)
        first = z_ref[0] * ny
        for y in range(ny):
            count = jnp.full((8, 128), counts_ref[first + y], jnp.int32).astype(jnp.float32)
            shares_ref[y] = count / whole
        for k, read in enumerate(reads):
            read.wait()
            for piece in range(k * pieces_of, (k + 1) * pieces_of):
                at = piece * rows * 128
                block = held[:, at : at + rows * 128].astype(jnp.float32).reshape(rows, 128)
                out[ALL_ORDER.index(piece % pairs), piece // pairs] = block.astype(jnp.bfloat16)
        for read in rest:
            read.wait()

    return pl.pallas_call(
        body,
        out_shape=[
            pltpu.VMEM((pairs, planes, rows, 128), jnp.bfloat16),
            pltpu.VMEM((ny, 8, 128), jnp.float32),
            pltpu.VMEM((rows, 128), momentum.dtype),
            pltpu.VMEM((rows, 128), params.dtype),
        ],
        in_specs=[SMEM, HBM, HBM, HBM, HBM],
        out_specs=[VMEM] * 4,
        scratch_shapes=[
            pltpu.VMEM(deltas.shape, deltas.dtype),
            pltpu.SMEM(counts.shape, counts.dtype),
            pltpu.SemaphoreType.DMA((READS + 3,)),
        ],
        name="prepared",
    )(z.reshape(1), counts, deltas, momentum, params)


def weighted(got, shares, old, was, z, nc):
    pairs, planes, rows, _ = got.shape

    def body(z_ref, shares_ref, got_ref, old_ref, was_ref, out_ref, own_ref):
        shares = [shares_ref[y][None] for y in range(pairs // nc)]
        for h in range(nc):
            for p in range(planes):
                acc = None
                for y, share in enumerate(shares):
                    term = got_ref[ALL_ORDER.index(y * nc + h), p].astype(jnp.float32).reshape(rows // 8, 8, 128)
                    term = share * term
                    acc = term if acc is None else acc + term
                out_ref[h * planes + p] = acc.reshape(rows, 128)
        z = z_ref[0]
        own = out_ref[z]
        own_ref[...] = own
        rest = was_ref[...].astype(jnp.float32) * (1 / grad_rate) - old_ref[...] * (old_rate / grad_rate)
        out_ref[z] = own - rest

    return pl.pallas_call(
        body,
        out_shape=[
            pltpu.VMEM((nc * planes, rows, 128), jnp.float32),
            pltpu.VMEM((rows, 128), jnp.float32),
        ],
        in_specs=[SMEM] + [VMEM] * 4,
        out_specs=[VMEM] * 2,
        name="weighted",
    )(z.reshape(1), *map(on_chip, (shares, got, old, was)))


def updated(every, own, old, z):
    planes, _, rows, _ = every.shape

    def body(z_ref, every_ref, own_ref, old_ref, momentum_ref, out_ref):
        z = z_ref[0]
        grad = own_ref[...]
        for step in range(1, planes):
            grad = grad + every_ref[(z + step) % planes, z]
        momentum_ref[...] = momentum_rate * old_ref[...] + grad
        for p in range(planes):
            total = every_ref[0, p]
            for k in range(1, planes):
                total = total + every_ref[k, p]
            out_ref[p] = (-grad_rate * total).astype(jnp.bfloat16)

    return pl.pallas_call(
        body,
        out_shape=[
            pltpu.VMEM((rows, 128), jnp.float32),
            pltpu.VMEM((planes, rows, 128), jnp.bfloat16),
        ],
        in_specs=[SMEM] + [VMEM] * 3,
        out_specs=[VMEM] * 2,
        name="updated",
    )(z.reshape(1), *map(on_chip, (every, own, old)))


def exchanged(x, groups):
    return lax.all_to_all(x, "yc", 0, 0, tiled=True, axis_index_groups=groups)


def local(deltas, counts, momentum, params):
    nz, nc = lax.axis_size("z"), CORES
    ny = lax.axis_size("yc") // nc
    z, c = lax.axis_index("z"), lax.axis_index("yc") % nc
    rows = momentum.shape[0] // 128

    pieces, shares, old, was = prepared(
        deltas, counts, momentum.reshape(rows, 128), params.reshape(rows, 128), z, ny, nc, nz
    )
    partial, mine = weighted(exchanged(pieces, [ALL_ORDER]), shares, old, was, z, nc)
    new_momentum, plane = updated(lax.all_gather(partial, "z"), mine, old, z)
    own = exchanged(jnp.broadcast_to(plane[None], (ny, *plane.shape)), SAME_CORE)
    other = lax.ppermute(own, "yc", [(i, i ^ 1) for i in range(ny * nc)])

    out = jnp.zeros((nz, ny, nc, rows, 128), jnp.bfloat16)
    for at, half in ((c, own), (1 - c, other)):
        bits = half.reshape(2, 2, 2, nz, rows, 128)
        block = jnp.transpose(bits, (3, 2, 1, 0, 4, 5)).reshape(nz, ny, 1, rows, 128)
        out = lax.dynamic_update_slice(out, block, (0, 0, at, 0, 0))
    return new_momentum.reshape(-1), out.reshape(-1)


def solution(mesh):
    torus = Mesh(mesh.devices.reshape(4, 16, mesh.shape["shard"]), ("z", "yc", "shard"))
    R = ("z", "yc")
    return jax.shard_map(
        local,
        mesh=torus,
        in_specs=(P(R, "shard"), P(), P(("shard",) + R), P(("shard",) + R)),
        out_specs=(P(("shard",) + R), P("shard")),
        check_vma=False,
    )
```

```python
import jax
import jax.numpy as jnp
from jax import lax
from jax.experimental import pallas as pl
from jax.experimental.pallas import tpu as pltpu
from jax.sharding import Mesh
from jax.sharding import PartitionSpec as P

momentum_rate = 0.9
outer_rate = 0.7
grad_rate = outer_rate * (1 + momentum_rate)
old_rate = outer_rate * momentum_rate * momentum_rate
READS = 4
Y_ORDER = (0, 4, 2, 6, 1, 5, 3, 7)
CORES = 2
FIRST_ORDER = (0, 4, 1, 5, 2, 6, 3, 7)
ALL_ORDER = [y * CORES + c for c in range(CORES) for y in FIRST_ORDER[:: 1 - 2 * c]]
SAME_CORE = [[y * CORES + c for y in Y_ORDER] for c in range(CORES)]

VMEM = pl.BlockSpec(memory_space=pltpu.VMEM)
SMEM = pl.BlockSpec(memory_space=pltpu.SMEM)
HBM = pl.BlockSpec(memory_space=pltpu.HBM)


def on_chip(x):
    return pltpu.with_memory_space_constraint(x, pltpu.VMEM)


def prepared(deltas, counts, momentum, params, z, ny, nc, nz):
    rows = momentum.shape[0]
    pairs, planes = ny * nc, nz // nc
    step = deltas.shape[1] // READS
    pieces_of = step // (rows * 128)
    workers = counts.shape[0]

    def body(z_ref, counts, src, old, was, out, shares_ref, old_ref, was_ref, held, counts_ref, sems):
        reads = [
            pltpu.make_async_copy(
                src.at[:, pl.ds(k * step, step)], held.at[:, pl.ds(k * step, step)], sems.at[k]
            )
            for k in range(READS)
        ]
        for read in reads:
            read.start()
        tokens = pltpu.make_async_copy(counts, counts_ref, sems.at[READS + 2])
        tokens.start()
        rest = [
            pltpu.make_async_copy(old, old_ref, sems.at[READS]),
            pltpu.make_async_copy(was, was_ref, sems.at[READS + 1]),
        ]
        for read in rest:
            read.start()
        tokens.wait()
        total = counts_ref[0]
        for w in range(1, workers):
            total += counts_ref[w]
        whole = jnp.full((8, 128), total, jnp.int32).astype(jnp.float32)
        first = z_ref[0] * ny
        for y in range(ny):
            count = jnp.full((8, 128), counts_ref[first + y], jnp.int32).astype(jnp.float32)
            shares_ref[y] = count / whole
        for k, read in enumerate(reads):
            read.wait()
            for piece in range(k * pieces_of, (k + 1) * pieces_of):
                at = piece * rows * 128
                block = held[:, at : at + rows * 128].astype(jnp.float32).reshape(rows, 128)
                out[ALL_ORDER.index(piece % pairs), piece // pairs] = block.astype(jnp.bfloat16)
        for read in rest:
            read.wait()

    return pl.pallas_call(
        body,
        out_shape=[
            pltpu.VMEM((pairs, planes, rows, 128), jnp.bfloat16),
            pltpu.VMEM((ny, 8, 128), jnp.float32),
            pltpu.VMEM((rows, 128), momentum.dtype),
            pltpu.VMEM((rows, 128), params.dtype),
        ],
        in_specs=[SMEM, HBM, HBM, HBM, HBM],
        out_specs=[VMEM] * 4,
        scratch_shapes=[
            pltpu.VMEM(deltas.shape, deltas.dtype),
            pltpu.SMEM(counts.shape, counts.dtype),
            pltpu.SemaphoreType.DMA((READS + 3,)),
        ],
        name="prepared",
    )(z.reshape(1), counts, deltas, momentum, params)


def weighted(got, shares, old, was, z, nc):
    pairs, planes, rows, _ = got.shape

    def body(z_ref, shares_ref, got_ref, old_ref, was_ref, out_ref, own_ref):
        shares = [shares_ref[y][None] for y in range(pairs // nc)]
        for h in range(nc):
            for p in range(planes):
                acc = None
                for y, share in enumerate(shares):
                    term = got_ref[ALL_ORDER.index(y * nc + h), p].astype(jnp.float32).reshape(rows // 8, 8, 128)
                    term = share * term
                    acc = term if acc is None else acc + term
                out_ref[h * planes + p] = acc.reshape(rows, 128)
        z = z_ref[0]
        own = out_ref[z]
        own_ref[...] = own
        rest = was_ref[...].astype(jnp.float32) * (1 / grad_rate) - old_ref[...] * (old_rate / grad_rate)
        out_ref[z] = own - rest

    return pl.pallas_call(
        body,
        out_shape=[
            pltpu.VMEM((nc * planes, rows, 128), jnp.float32),
            pltpu.VMEM((rows, 128), jnp.float32),
        ],
        in_specs=[SMEM] + [VMEM] * 4,
        out_specs=[VMEM] * 2,
        name="weighted",
    )(z.reshape(1), *map(on_chip, (shares, got, old, was)))


def updated(every, own, old, z):
    planes, _, rows, _ = every.shape

    def body(z_ref, every_ref, own_ref, old_ref, momentum_ref, out_ref):
        z = z_ref[0]
        grad = own_ref[...]
        for step in range(1, planes):
            grad = grad + every_ref[(z + step) % planes, z]
        momentum_ref[...] = momentum_rate * old_ref[...] + grad
        for p in range(planes):
            total = every_ref[0, p]
            for k in range(1, planes):
                total = total + every_ref[k, p]
            out_ref[p] = (-grad_rate * total).astype(jnp.bfloat16)

    return pl.pallas_call(
        body,
        out_shape=[
            pltpu.VMEM((rows, 128), jnp.float32),
            pltpu.VMEM((planes, rows, 128), jnp.bfloat16),
        ],
        in_specs=[SMEM] + [VMEM] * 3,
        out_specs=[VMEM] * 2,
        name="updated",
    )(z.reshape(1), *map(on_chip, (every, own, old)))


def exchanged(x, groups):
    return lax.all_to_all(x, "yc", 0, 0, tiled=True, axis_index_groups=groups)


def local(deltas, counts, momentum, params):
    nz, nc = lax.axis_size("z"), CORES
    ny = lax.axis_size("yc") // nc
    z, c = lax.axis_index("z"), lax.axis_index("yc") % nc
    rows = momentum.shape[0] // 128

    pieces, shares, old, was = prepared(
        deltas, counts, momentum.reshape(rows, 128), params.reshape(rows, 128), z, ny, nc, nz
    )
    partial, mine = weighted(exchanged(pieces, [ALL_ORDER]), shares, old, was, z, nc)
    new_momentum, plane = updated(lax.all_gather(partial, "z"), mine, old, z)
    own = exchanged(jnp.broadcast_to(plane[None], (ny, *plane.shape)), SAME_CORE)
    other = lax.ppermute(own, "yc", [(i, i ^ 1) for i in range(ny * nc)])

    out = jnp.zeros((nz, ny, nc, rows, 128), jnp.bfloat16)
    for at, half in ((c, own), (1 - c, other)):
        bits = half.reshape(2, 2, 2, nz, rows, 128)
        block = jnp.transpose(bits, (3, 2, 1, 0, 4, 5)).reshape(nz, ny, 1, rows, 128)
        out = lax.dynamic_update_slice(out, block, (0, 0, at, 0, 0))
    return new_momentum.reshape(-1), out.reshape(-1)


def solution(mesh):
    torus = Mesh(mesh.devices.reshape(4, 16, mesh.shape["shard"]), ("z", "yc", "shard"))
    R = ("z", "yc")
    return jax.shard_map(
        local,
        mesh=torus,
        in_specs=(P(R, "shard"), P(), P(("shard",) + R), P(("shard",) + R)),
        out_specs=(P(("shard",) + R), P("shard")),
        check_vma=False,
    )
```
